32 devices in a mesh: dp: 8 (over z, core), tp: 4 (over y, x).
Axes of the slice: x: 2, y: 2, z: 4, core: 2. Of those that a mesh axis runs over, the one named last changes fastest.
Arguments:
- hidden_states: bfloat16 [2048, 3584], P('dp'), may hold values from -21 to 21
- resp_lengths: int32 [4], replicated, may hold values from 1 to 1280, 2048 in all
- w_query: bfloat16 [3584, 512], P('dp', 'tp'), may hold values from -0.25 to 0.25
- w_keyval: bfloat16 [3584, 1024], P('dp', 'tp'), may hold values from -0.09375 to 0.09375
- w_out: bfloat16 [512, 3584], P('tp', 'dp'), may hold values from -0.25 to 0.25
Outputs:
- attended: bfloat16 [2048, 3584], P('dp', 'tp')
The draws below stay inside these ranges and needn't reach their ends.
Inputs may be any that keep to these rules, and one draw needn't show every extreme that they name: `resp_lengths`: the 4 lengths sum to 2048; the longest is exactly 1280.
All inputs are finite; a program needn't handle non-finite values.
Results may differ from the reference program's by a relative error of at most 0.015.
The reference program's roundings to bfloat16 on the way count: a program that leaves them out, or rounds other values in their place, can miss the bound.
Values may be sent and summed in bfloat16 or wider, within the bound.
A program may use at most 64 MiB of HBM per device.

```python
import math
import jax
import jax.numpy as jnp
import numpy as np
from jax import lax

D = 3584
HD = 128
KV = 4
TOK_DEV = 256
HEADS = 4
TOKENS = 2048
LMAX = 1280
NRESP = 4
N_TP = 4


def draw_hidden_states(key, part):
    first_key = jax.random.fold_in(jax.random.fold_in(key, 11), 0)
    values = jnp.clip(jax.random.normal(first_key, (TOKENS, D), jnp.float32), -6.0, 6.0)
    return values.astype(jnp.bfloat16)


def level_of(stream_key, extent, shards, low, high):
    factor_of = 1.0
    for dim, parts in shards:
        draws = jax.random.uniform(jax.random.fold_in(jax.random.fold_in(stream_key, 6), dim), (parts,), jnp.float32, low / len(shards), high / len(shards))
        factor_of = factor_of * jnp.repeat(jnp.exp(draws), extent[dim] // parts).reshape((-1,) + (1,) * (len(extent) - 1 - dim))
    return factor_of


def length_profile(amount, total, reach, slope):
    portions = [(1 << 20) // math.isqrt(grade ** slope) + 1 for grade in range(2, amount + 1)]
    surplus, holding = total - reach - (amount - 1), [1] * (amount - 1)
    while surplus > 0:
        free = [i for i in range(amount - 1) if holding[i] < reach]
        whole, budget = sum([portions[i] for i in free]), surplus
        for i in free:
            extra = min(reach - holding[i], max(1, budget * portions[i] // whole), surplus)
            holding[i] = holding[i] + extra
            surplus = surplus - extra
    return np.array([reach] + holding)


def uneven_parts(own_key, amount, total, limit, skew):
    if amount == 2:
        one = jax.random.randint(own_key, (), max(1, total - limit), min(limit, total - 1) + 1)
        return jnp.stack([one, total - one])
    tallies = jnp.asarray(length_profile(amount, total, limit, skew), jnp.int32)
    couples = (amount - 1) // 2
    donor, sink = tallies[1:1 + 2 * couples:2], tallies[2:2 + 2 * couples:2]
    room = jnp.minimum(donor - 1, limit - sink)
    moved = jax.random.randint(jax.random.fold_in(own_key, 1), (couples,), 0, 1 << 20) % (room + 1)
    tallies = tallies.at[1:1 + 2 * couples:2].set(donor - moved).at[2:2 + 2 * couples:2].set(sink + moved)
    return tallies[jax.random.permutation(jax.random.fold_in(own_key, 2), amount)]


def centred(own_key, shape, width, reach, pieces=(), kind=jnp.bfloat16):
    result = width * jax.random.normal(own_key, shape, jnp.float32)
    if pieces:
        result = result * level_of(own_key, shape, pieces, -0.22, 0.18)
    return jnp.clip(result, -reach, reach).astype(kind)


def setup_inputs(seed: int = 0) -> dict:
    key_list = jax.random.split(jax.random.key(seed), 6)
    hidden_states = draw_hidden_states(jax.random.fold_in(key_list[5], 71), 0)
    resp_lengths = uneven_parts(key_list[1], NRESP, TOKENS, LMAX, 2).astype(jnp.int32)
    w_query = centred(key_list[2], (D, HEADS * HD), (D // 6) ** -0.5, 0.25, ((0, 8), (1, 4)))
    w_keyval = centred(key_list[3], (D, 2 * KV * HD), D ** -0.5, 0.09375, ((0, 8), (1, 4)))
    w_out = centred(key_list[4], (HEADS * HD, D), (HEADS * HD) ** -0.5, 0.25, ((0, 4), (1, 8)))
    return dict(hidden_states=hidden_states, resp_lengths=resp_lengths, w_query=w_query, w_keyval=w_keyval, w_out=w_out)


def reference(hidden_states, resp_lengths, w_query, w_keyval, w_out):
    total_tokens = hidden_states.shape[0]
    head_scale = HD ** -0.5
    query = (jnp.dot(hidden_states, w_query, preferred_element_type=jnp.float32) * head_scale).astype(jnp.bfloat16)
    keyval = jnp.dot(hidden_states, w_keyval, preferred_element_type=jnp.float32).astype(jnp.bfloat16)
    resp_ends = jnp.cumsum(resp_lengths, dtype=jnp.int32)
    position = jnp.arange(total_tokens, dtype=jnp.int32)
    segment = jnp.sum((position[:, None] >= resp_ends[None, :]).astype(jnp.int32), axis=1, dtype=jnp.int32)
    window = min(total_tokens, TOK_DEV + LMAX)
    blocks = total_tokens // TOK_DEV
    per_group = HEADS // KV

    def one_head(head):
        kv_head = (head // per_group).astype(jnp.int32)
        key_head = lax.dynamic_slice_in_dim(keyval, kv_head * HD, HD, 1)
        value_head = lax.dynamic_slice_in_dim(keyval, (KV + kv_head) * HD, HD, 1)
        query_head = lax.dynamic_slice_in_dim(query, (head * HD).astype(jnp.int32), HD, 1)

        def one_block(block):
            begin = (block * TOK_DEV).astype(jnp.int32)
            key_begin = jnp.clip(begin + TOK_DEV - window, 0, total_tokens - window).astype(jnp.int32)
            query_rows = lax.dynamic_slice_in_dim(query_head, begin, TOK_DEV, 0)
            key_rows = lax.dynamic_slice_in_dim(key_head, key_begin, window, 0)
            value_rows = lax.dynamic_slice_in_dim(value_head, key_begin, window, 0)
            query_pos = begin + jnp.arange(TOK_DEV, dtype=jnp.int32)
            key_pos = key_begin + jnp.arange(window, dtype=jnp.int32)
            query_seg = lax.dynamic_slice_in_dim(segment, begin, TOK_DEV, 0)
            key_seg = lax.dynamic_slice_in_dim(segment, key_begin, window, 0)
            scores = jnp.dot(query_rows, key_rows.T, preferred_element_type=jnp.float32)
            allowed = (query_seg[:, None] == key_seg[None, :]) & (key_pos[None, :] <= query_pos[:, None])
            largest = jnp.max(jnp.where(allowed, scores, jnp.float32(-1e30)), axis=1)
            expw = jnp.where(allowed, jnp.exp(scores - largest[:, None]), jnp.float32(0.0))
            denom = jnp.sum(expw, axis=1)
            numer = jnp.dot(expw.astype(jnp.bfloat16), value_rows, preferred_element_type=jnp.float32)
            return (numer / denom[:, None]).astype(jnp.bfloat16)

        return lax.map(one_block, jnp.arange(blocks, dtype=jnp.int32)).reshape(total_tokens, HD)

    heads_all = lax.map(one_head, jnp.arange(HEADS, dtype=jnp.int32))
    heads_out = jnp.transpose(heads_all, (1, 0, 2)).reshape(total_tokens, HEADS * HD)
    group_width = (HEADS // N_TP) * HD
    summed = jnp.zeros((total_tokens, w_out.shape[1]), jnp.float32)
    for group in range(N_TP):
        partial_sum = jnp.dot(heads_out[:, group * group_width:(group + 1) * group_width],
                              w_out[group * group_width:(group + 1) * group_width],
                              preferred_element_type=jnp.float32).astype(jnp.bfloat16)
        partial_sum = lax.optimization_barrier(partial_sum)
        summed = summed + partial_sum.astype(jnp.float32)
    return summed.astype(jnp.bfloat16)
```

```python
import functools

import jax
import jax.numpy as jnp
from jax import lax
from jax.experimental import pallas as pl
from jax.experimental.pallas import tpu as pltpu
from jax.sharding import PartitionSpec as P

HD = 128


def segment_of(position, resp_ends):
    return jnp.sum(
        (position[:, None] >= resp_ends[None, :]).astype(jnp.int32), axis=1, dtype=jnp.int32
    )


def body(hidden_states, resp_lengths, w_query, w_keyval, w_out):
    token_rows = hidden_states.shape[0]
    head_scale = HD ** (-0.5)
    pieces = (
        lax.all_gather(w_query, "dp", axis=0, tiled=True),
        lax.all_gather(w_keyval, "dp", axis=0, tiled=True),
    )
    query_sum = jnp.dot(hidden_states, pieces[0], preferred_element_type=jnp.float32)
    keyval_sum = jnp.dot(hidden_states, pieces[1], preferred_element_type=jnp.float32)
    query = (query_sum * head_scale).astype(jnp.bfloat16)
    keyval = lax.all_gather(keyval_sum.astype(jnp.bfloat16), "tp", axis=1, tiled=True)
    kv_count = keyval.shape[1] // (2 * HD)
    per_group = lax.axis_size("tp") // kv_count
    kv_head = lax.axis_index("tp") // per_group
    key_head = lax.dynamic_slice_in_dim(keyval, kv_head * HD, HD, 1)
    value_head = lax.dynamic_slice_in_dim(keyval, (kv_count + kv_head) * HD, HD, 1)
    head_pair = jnp.concatenate([key_head, value_head], axis=1)
    resp_ends = jnp.cumsum(resp_lengths, dtype=jnp.int32)
    own_begin = lax.axis_index("dp") * token_rows
    query_pos = own_begin + jnp.arange(token_rows, dtype=jnp.int32)
    query_seg = segment_of(query_pos, resp_ends)
    pieces = lax.all_gather(head_pair, "dp", axis=0, tiled=True)
    largest = jnp.full((token_rows,), -1e30, jnp.float32)
    height = pieces.shape[0]
    key_pos = jnp.arange(height, dtype=jnp.int32)
    key_seg = segment_of(key_pos, resp_ends)
    scores = jnp.dot(query, pieces[:, :HD].T, preferred_element_type=jnp.float32)
    allowed = (
        (query_seg[:, None] == key_seg[None, :])
        & (key_pos[None, :] <= query_pos[:, None])
        & (key_pos[None, :] >= 0)
    )
    newest = jnp.maximum(largest, jnp.max(jnp.where(allowed, scores, jnp.float32(-1e30)), axis=1))
    expw = jnp.where(allowed, jnp.exp(scores - newest[:, None]), jnp.float32(0.0))
    denom = jnp.sum(expw, axis=1)
    numer = jnp.dot(expw.astype(jnp.bfloat16), pieces[:, HD:], preferred_element_type=jnp.float32)
    heads_out = (numer / denom[:, None]).astype(jnp.bfloat16)
    terms = jnp.dot(
        heads_out,
        lax.all_gather(w_out, "dp", axis=1, tiled=True),
        preferred_element_type=jnp.float32,
    )
    summed = lax.psum_scatter(terms.astype(jnp.bfloat16), "tp", scatter_dimension=1, tiled=True)
    return summed


MESH = pl.DeviceIdType.MESH
KVA, KVB, WQ, WO, KD = range(5)


def fused_kernel(
    nz, nt, lens_ref, hid_hbm, wq_hbm, wkv_hbm, wo_hbm, out_ref,
    hid, wq, wkv, woc, wof, kvloc, kvb, kvacc, qacc, qbuf, scores, mref, lref, oacc, hloc, hcat,
    loc_sem, ss, rs, prs, kv_ss, kv_rs, wi_ss, wi_rs, wp_ss, wp_rs, h_ss, h_rs,
):
    dp = lax.axis_index("dp")
    t = lax.axis_index("tp")
    z, c = dp // 2, dp % 2
    rows = hid.shape[0]
    shard = wq_hbm.shape[0]
    half = shard // 2
    nout = wo_hbm.shape[1]

    loads = [
        pltpu.make_async_copy(wkv_hbm, wkv.at[pl.ds(dp * shard, shard)], loc_sem.at[0]),
        pltpu.make_async_copy(wq_hbm, wq.at[pl.ds(dp * shard, shard)], loc_sem.at[1]),
        pltpu.make_async_copy(hid_hbm, hid, loc_sem.at[2]),
        pltpu.make_async_copy(wo_hbm, woc.at[z], loc_sem.at[3]),
    ]
    for load in loads:
        load.start()

    barrier = pltpu.get_barrier_semaphore()
    partner = {"dp": dp + 1 - 2 * c, "tp": t}
    up, down = {"dp": dp + 2, "tp": t}, {"dp": dp - 2, "tp": t}
    has_up, has_down = z < nz - 1, z > 0
    pl.semaphore_signal(barrier, 1, device_id=partner, device_id_type=MESH)

    @pl.when(has_up)
    def _():
        pl.semaphore_signal(barrier, 1, device_id=up, device_id_type=MESH)

    @pl.when(has_down)
    def _():
        pl.semaphore_signal(barrier, 1, device_id=down, device_id_type=MESH)

    for k in range(1, nt):
        pl.semaphore_signal(
            barrier, 1, device_id={"dp": dp, "tp": (t + k) % nt}, device_id_type=MESH
        )
    pl.semaphore_wait(barrier, nt + has_up.astype(jnp.int32) + has_down.astype(jnp.int32))

    def slot(item, zz, cc):
        if item == KVA:
            return wkv.at[pl.ds((2 * zz + cc) * shard, half)]
        if item == KVB:
            return wkv.at[pl.ds((2 * zz + cc) * shard + half, half)]
        if item == WQ:
            return wq.at[pl.ds((2 * zz + cc) * shard, shard)]
        if item == WO:
            return woc.at[zz]
        return kvb.at[2 * zz + cc]

    def chain(item, zz, way):
        ref = slot(item, zz, c)
        if way == 2:
            recv, to = prs.at[item, zz], partner
        else:
            recv, to = rs.at[item, zz], (up if way == 0 else down)
        return pltpu.make_async_remote_copy(
            ref, ref, ss.at[item, zz, way], recv, device_id=to, device_id_type=MESH
        )

    def from_chain(item, zz):
        ref = slot(item, zz, c)
        pltpu.make_async_remote_copy(
            ref, ref, ss.at[item, zz, 0], rs.at[item, zz], device_id=partner, device_id_type=MESH
        ).wait_recv()

    def from_partner(item, zz):
        ref = slot(item, zz, 1 - c)
        pltpu.make_async_remote_copy(
            ref, ref, ss.at[item, zz, 2], prs.at[item, zz], device_id=partner, device_id_type=MESH
        ).wait_recv()

    def own_moves(item, act):
        @pl.when(has_up)
        def _():
            act(chain(item, z, 0))

        if item != KD:
            @pl.when(has_down)
            def _():
                act(chain(item, z, 1))

        if item == KD:
            @pl.when(c == 0)
            def _():
                act(chain(item, z, 2))
        elif item != WO:
            act(chain(item, z, 2))

    def passed_moves(item, k, below, act):
        zz = z - k if below else z + k
        if below:
            @pl.when(has_up)
            def _():
                act(chain(item, zz, 0))
        else:
            @pl.when(has_down)
            def _():
                act(chain(item, zz, 1))
        if item != WO:
            act(chain(item, zz, 2))

    def start(copy):
        copy.start()

    def wait_send(copy):
        copy.wait_send()

    def in_plane(zz):
        return pltpu.make_async_remote_copy(
            woc.at[zz], wof.at[c, pl.ds(t * HD, HD)], wi_ss.at[zz], wi_rs.at[t],
            device_id={"dp": dp, "tp": zz}, device_id_type=MESH,
        )

    def take_wo(zz):
        @pl.when(zz != t)
        def _():
            in_plane(zz).start()

        @pl.when(zz == t)
        def _():
            wof[c, pl.ds(pl.multiple_of(t * HD, HD), HD), :] = woc[zz]
            own_wo(zz).start()

    def own_wo(zz):
        return pltpu.make_async_remote_copy(
            woc.at[zz], wof.at[c, pl.ds(t * HD, HD)], wp_ss.at[t], wp_rs.at[t],
            device_id=partner, device_id_type=MESH,
        )

    def pass_on(item, k):
        @pl.when(z - k >= 0)
        def _():
            from_chain(item, z - k)
            passed_moves(item, k, True, start)
            if item == WO:
                take_wo(z - k)

        if item != KD:
            @pl.when(z + k < nz)
            def _():
                from_chain(item, z + k)
                passed_moves(item, k, False, start)
                if item == WO:
                    take_wo(z + k)

    def each_side(k, fn):
        @pl.when(z - k >= 0)
        def _():
            fn(z - k)

        @pl.when(z + k < nz)
        def _():
            fn(z + k)

    def hidden_part(zz):
        return hid[:, pl.ds(pl.multiple_of(zz * 2 * shard, 128), 2 * shard)]

    def add_kv(zz):
        from_partner(KVA, zz)
        from_partner(KVB, zz)
        weights = wkv[pl.ds(pl.multiple_of(zz * 2 * shard, 16), 2 * shard), :]
        kvacc[...] += jnp.dot(hidden_part(zz), weights, preferred_element_type=jnp.float32)

    def add_q(zz):
        from_partner(WQ, zz)
        weights = wq[pl.ds(pl.multiple_of(zz * 2 * shard, 16), 2 * shard), :]
        qacc[...] += jnp.dot(hidden_part(zz), weights, preferred_element_type=jnp.float32)

    loads[0].wait()
    own_moves(KVA, start)
    own_moves(KVB, start)
    loads[1].wait()
    loads[2].wait()
    loads[3].wait()
    kvacc[...] = jnp.zeros_like(kvacc)
    qacc[...] = jnp.zeros_like(qacc)
    add_kv(z)
    for k in range(1, nz):
        pass_on(KVA, k)
        pass_on(KVB, k)
        if k == nz - 1:
            own_moves(WQ, start)
        each_side(k, add_kv)

    role = t // (nt // 2)
    for h in range(2):
        kvloc[h] = kvacc[:, h * HD:(h + 1) * HD].astype(jnp.bfloat16)

    def kv_send(h):
        return pltpu.make_async_remote_copy(
            kvloc.at[h], kvb.at[dp, role], kv_ss.at[h], kv_rs.at[role],
            device_id={"dp": dp, "tp": 2 * (t % (nt // 2)) + h}, device_id_type=MESH,
        )

    for h in range(2):
        to = 2 * (t % (nt // 2)) + h

        @pl.when(to != t)
        def _():
            kv_send(h).start()

        @pl.when(to == t)
        def _():
            kvb[dp, role] = kvloc[h]

    add_q(z)
    for k in range(1, nz):
        pass_on(WQ, k)
        if k == 1:
            for r in range(2):
                @pl.when(t // 2 + r * (nt // 2) != t)
                def _():
                    pltpu.make_async_remote_copy(
                        kvloc.at[r], kvb.at[dp, r], kv_ss.at[r], kv_rs.at[r],
                        device_id=partner, device_id_type=MESH,
                    ).wait_recv()

            own_moves(KD, start)

            @pl.when(c == 0)
            def _():
                kvb[dp + 1] = jnp.zeros(kvb.shape[1:], kvb.dtype)

        if k == nz - 1:
            own_moves(WO, start)
            take_wo(z)
        each_side(k, add_q)
    qbuf[...] = (qacc[...] * (HD ** -0.5)).astype(jnp.bfloat16)

    qpos = dp * rows + lax.broadcasted_iota(jnp.int32, (rows, 1), 0)
    first = jnp.zeros((rows, 1), jnp.int32)
    end = jnp.int32(0)
    for r in range(lens_ref.shape[0]):
        end = end + lens_ref[r]
        first = jnp.where(qpos >= end, end, first)

    def pair(zz, which):
        return jnp.concatenate([kvb[2 * zz, which], kvb[2 * zz + 1, which]], axis=0)

    def score(zz):
        s = lax.dot_general(
            qbuf[...], pair(zz, 0), (((1,), (1,)), ((), ())), preferred_element_type=jnp.float32
        )
        kpos = zz * 2 * rows + lax.broadcasted_iota(jnp.int32, s.shape, 1)
        s = jnp.where((kpos >= first) & (kpos <= qpos), s, jnp.float32(-1e30))
        scores[zz] = s
        mref[...] = jnp.maximum(mref[...], jnp.max(s, axis=1, keepdims=True))

    mref[...] = jnp.full_like(mref, -1e30)
    for k in range(nz):
        if k == 0:
            @pl.when(c == 1)
            def _():
                from_partner(KD, z)
            score(z)
        else:
            pass_on(KD, k)
            pass_on(WO, k)

            @pl.when(z - k >= 0)
            def _():
                from_partner(KD, z - k)
                score(z - k)

    lref[...] = jnp.zeros_like(lref)
    oacc[...] = jnp.zeros_like(oacc)

    def weigh(zz):
        p = jnp.exp(scores[zz] - mref[...])
        lref[...] += jnp.sum(p, axis=1, keepdims=True)
        oacc[...] += jnp.dot(p.astype(jnp.bfloat16), pair(zz, 1), preferred_element_type=jnp.float32)

    for k in range(nz):
        @pl.when(z - k >= 0)
        def _():
            weigh(z - k)

    heads = (oacc[...] / lref[...]).astype(jnp.bfloat16)
    hloc[...] = heads
    hcat[t] = heads

    def head_copy(k):
        return pltpu.make_async_remote_copy(
            hloc, hcat.at[t], h_ss.at[k], h_rs.at[t],
            device_id={"dp": dp, "tp": (t + k) % nt}, device_id_type=MESH,
        )

    for k in range(1, nt):
        head_copy(k).start()

    def wo_block(g, cc):
        return wof.at[cc, pl.ds(g * HD, HD)]

    def wo_partner(g):
        return pltpu.make_async_remote_copy(
            wo_block(g, c), wo_block(g, c), wp_ss.at[g], wp_rs.at[g],
            device_id=partner, device_id_type=MESH,
        )

    for k in range(1, nt):
        g = (t + k) % nt
        pltpu.make_async_remote_copy(
            woc.at[0], wo_block(g, c), wi_ss.at[0], wi_rs.at[g],
            device_id=partner, device_id_type=MESH,
        ).wait_recv()
        wo_partner(g).start()
    for g in range(nt):
        pltpu.make_async_remote_copy(
            woc.at[0], wo_block(g, 1 - c), wp_ss.at[g], wp_rs.at[g],
            device_id=partner, device_id_type=MESH,
        ).wait_recv()
    for k in range(1, nt):
        g = (t + k) % nt
        pltpu.make_async_remote_copy(
            hloc, hcat.at[g], h_ss.at[k], h_rs.at[g], device_id=partner, device_id_type=MESH
        ).wait_recv()
    every = jnp.concatenate([hcat[g] for g in range(nt)], axis=1)
    for cc in range(2):
        out_ref[:, cc * nout:(cc + 1) * nout] = jnp.dot(
            every, wof[cc], preferred_element_type=jnp.float32
        ).astype(out_ref.dtype)

    for item in (KVA, KVB, WQ, WO, KD):
        own_moves(item, wait_send)
        for k in range(1, nz):
            @pl.when(z - k >= 0)
            def _():
                passed_moves(item, k, True, wait_send)

            if item != KD:
                @pl.when(z + k < nz)
                def _():
                    passed_moves(item, k, False, wait_send)
    for h in range(2):
        @pl.when(2 * (t % (nt // 2)) + h != t)
        def _():
            kv_send(h).wait_send()
    for k in range(1, nt):
        head_copy(k).wait_send()
        wo_partner((t + k) % nt).wait_send()
        in_plane((t + k) % nt).wait_send()
    own_wo(t).wait_send()


def fused_body(nz, nt, hidden_states, resp_lengths, w_query, w_keyval, w_out):
    rows, depth = hidden_states.shape
    nout = w_out.shape[1]
    bf16, f32 = jnp.bfloat16, jnp.float32
    dma = pltpu.SemaphoreType.DMA
    hbm = pl.BlockSpec(memory_space=pltpu.HBM)
    return pl.pallas_call(
        functools.partial(fused_kernel, nz, nt),
        out_shape=jax.ShapeDtypeStruct((rows, 2 * nout), bf16),
        in_specs=[pl.BlockSpec(memory_space=pltpu.SMEM), hbm, hbm, hbm, hbm],
        out_specs=pl.BlockSpec(memory_space=pltpu.VMEM),
        scratch_shapes=[
            pltpu.VMEM((rows, depth), bf16),
            pltpu.VMEM((depth, w_query.shape[1]), bf16),
            pltpu.VMEM((depth, w_keyval.shape[1]), bf16),
            pltpu.VMEM((nz, HD, nout), bf16),
            pltpu.VMEM((2, nt * HD, nout), bf16),
            pltpu.VMEM((2, rows, HD), bf16),
            pltpu.VMEM((2 * nz, 2, rows, HD), bf16),
            pltpu.VMEM((rows, 2 * HD), f32),
            pltpu.VMEM((rows, HD), f32),
            pltpu.VMEM((rows, HD), bf16),
            pltpu.VMEM((nz, rows, 2 * rows), f32),
            pltpu.VMEM((rows, 1), f32),
            pltpu.VMEM((rows, 1), f32),
            pltpu.VMEM((rows, HD), f32),
            pltpu.VMEM((rows, HD), bf16),
            pltpu.VMEM((nt, rows, HD), bf16),
            dma((4,)),
            dma((5, nz, 3)),
            dma((5, nz)),
            dma((5, nz)),
            dma((2,)),
            dma((2,)),
            dma((nz,)),
            dma((nt,)),
            dma((nt,)),
            dma((nt,)),
            dma((nt,)),
            dma((nt,)),
        ],
        compiler_params=pltpu.CompilerParams(
            collective_id=0, has_side_effects=True, vmem_limit_bytes=50 * 1024 * 1024
        ),
    )(resp_lengths, hidden_states, w_query, w_keyval, w_out)


def per_device(mesh, hidden_states, resp_lengths, w_query, w_keyval, w_out):
    nt = mesh.shape["tp"]
    nz = mesh.shape["dp"] // 2
    args = (hidden_states, resp_lengths, w_query, w_keyval, w_out)
    fits = (
        mesh.shape["dp"] == 2 * nz and nz == nt and nt % 2 == 0
        and w_query.shape[1] == HD and w_keyval.shape[1] == 2 * HD
        and w_out.shape[0] == HD and w_query.shape[0] % 64 == 0
    )
    return fused_body(nz, nt, *args) if fits else body(*args)


def solution(mesh):
    return jax.shard_map(
        functools.partial(per_device, mesh),
        mesh=mesh,
        in_specs=(P("dp", None), P(), P("dp", "tp"), P("dp", "tp"), P("tp", "dp")),
        out_specs=P("dp", "tp"),
        check_vma=False,
    )
```

```python
import functools

import jax
import jax.numpy as jnp
from jax import lax
from jax.experimental import pallas as pl
from jax.experimental.pallas import tpu as pltpu
from jax.sharding import PartitionSpec as P

HD = 128


def segment_of(position, resp_ends):
    return jnp.sum(
        (position[:, None] >= resp_ends[None, :]).astype(jnp.int32), axis=1, dtype=jnp.int32
    )


def body(hidden_states, resp_lengths, w_query, w_keyval, w_out):
    token_rows = hidden_states.shape[0]
    head_scale = HD ** (-0.5)
    pieces = (
        lax.all_gather(w_query, "dp", axis=0, tiled=True),
        lax.all_gather(w_keyval, "dp", axis=0, tiled=True),
    )
    query_sum = jnp.dot(hidden_states, pieces[0], preferred_element_type=jnp.float32)
    keyval_sum = jnp.dot(hidden_states, pieces[1], preferred_element_type=jnp.float32)
    query = (query_sum * head_scale).astype(jnp.bfloat16)
    keyval = lax.all_gather(keyval_sum.astype(jnp.bfloat16), "tp", axis=1, tiled=True)
    kv_count = keyval.shape[1] // (2 * HD)
    per_group = lax.axis_size("tp") // kv_count
    kv_head = lax.axis_index("tp") // per_group
    key_head = lax.dynamic_slice_in_dim(keyval, kv_head * HD, HD, 1)
    value_head = lax.dynamic_slice_in_dim(keyval, (kv_count + kv_head) * HD, HD, 1)
    head_pair = jnp.concatenate([key_head, value_head], axis=1)
    resp_ends = jnp.cumsum(resp_lengths, dtype=jnp.int32)
    own_begin = lax.axis_index("dp") * token_rows
    query_pos = own_begin + jnp.arange(token_rows, dtype=jnp.int32)
    query_seg = segment_of(query_pos, resp_ends)
    pieces = lax.all_gather(head_pair, "dp", axis=0, tiled=True)
    largest = jnp.full((token_rows,), -1e30, jnp.float32)
    height = pieces.shape[0]
    key_pos = jnp.arange(height, dtype=jnp.int32)
    key_seg = segment_of(key_pos, resp_ends)
    scores = jnp.dot(query, pieces[:, :HD].T, preferred_element_type=jnp.float32)
    allowed = (
        (query_seg[:, None] == key_seg[None, :])
        & (key_pos[None, :] <= query_pos[:, None])
        & (key_pos[None, :] >= 0)
    )
    newest = jnp.maximum(largest, jnp.max(jnp.where(allowed, scores, jnp.float32(-1e30)), axis=1))
    expw = jnp.where(allowed, jnp.exp(scores - newest[:, None]), jnp.float32(0.0))
    denom = jnp.sum(expw, axis=1)
    numer = jnp.dot(expw.astype(jnp.bfloat16), pieces[:, HD:], preferred_element_type=jnp.float32)
    heads_out = (numer / denom[:, None]).astype(jnp.bfloat16)
    terms = jnp.dot(
        heads_out,
        lax.all_gather(w_out, "dp", axis=1, tiled=True),
        preferred_element_type=jnp.float32,
    )
    summed = lax.psum_scatter(terms.astype(jnp.bfloat16), "tp", scatter_dimension=1, tiled=True)
    return summed


MESH = pl.DeviceIdType.MESH
KVA, KVB, WQ, WO, KEY, VAL = range(6)


def fused_kernel(
    nz, nt, lens_ref, hid_hbm, wq_hbm, wkv_hbm, wo_hbm, out_ref,
    hid, wq, wkv, woc, wof, kvloc, kvb, kvacc, qacc, qbuf, scores, mref, lref, oacc, hloc, hcat,
    loc_sem, ss, rs, prs, kv_ss, kv_rs, wi_ss, wi_rs, wp_ss, wp_rs, h_ss, h_rs,
):
    dp = lax.axis_index("dp")
    t = lax.axis_index("tp")
    z, c = dp // 2, dp % 2
    rows = hid.shape[0]
    shard = wq_hbm.shape[0]
    half = shard // 2
    nout = wo_hbm.shape[0]

    loads = [
        pltpu.make_async_copy(wkv_hbm, wkv.at[pl.ds(dp * shard, shard)], loc_sem.at[0]),
        pltpu.make_async_copy(wq_hbm, wq.at[pl.ds(dp * shard, shard)], loc_sem.at[1]),
        pltpu.make_async_copy(hid_hbm, hid, loc_sem.at[2]),
        pltpu.make_async_copy(wo_hbm, woc.at[z], loc_sem.at[3]),
    ]
    for load in loads:
        load.start()

    barrier = pltpu.get_barrier_semaphore()
    partner = {"dp": dp + 1 - 2 * c, "tp": t}
    up, down = {"dp": dp + 2, "tp": t}, {"dp": dp - 2, "tp": t}
    has_up, has_down = z < nz - 1, z > 0
    pl.semaphore_signal(barrier, 1, device_id=partner, device_id_type=MESH)

    @pl.when(has_up)
    def _():
        pl.semaphore_signal(barrier, 1, device_id=up, device_id_type=MESH)

    @pl.when(has_down)
    def _():
        pl.semaphore_signal(barrier, 1, device_id=down, device_id_type=MESH)

    for k in range(1, nt):
        pl.semaphore_signal(
            barrier, 1, device_id={"dp": dp, "tp": (t + k) % nt}, device_id_type=MESH
        )
    pl.semaphore_wait(barrier, nt + has_up.astype(jnp.int32) + has_down.astype(jnp.int32))

    def slot(item, zz, cc):
        if item == KVA:
            return wkv.at[pl.ds((2 * zz + cc) * shard, half)]
        if item == KVB:
            return wkv.at[pl.ds((2 * zz + cc) * shard + half, half)]
        if item == WQ:
            return wq.at[pl.ds((2 * zz + cc) * shard, shard)]
        if item == WO:
            return woc.at[zz]
        return kvb.at[2 * zz + cc, 0 if item == KEY else 1]

    def chain(item, zz, way):
        ref = slot(item, zz, c)
        if way == 2:
            recv, to = prs.at[item, zz], partner
        else:
            recv, to = rs.at[item, zz], (up if way == 0 else down)
        return pltpu.make_async_remote_copy(
            ref, ref, ss.at[item, zz, way], recv, device_id=to, device_id_type=MESH
        )

    def from_chain(item, zz):
        ref = slot(item, zz, c)
        pltpu.make_async_remote_copy(
            ref, ref, ss.at[item, zz, 0], rs.at[item, zz], device_id=partner, device_id_type=MESH
        ).wait_recv()

    def from_partner(item, zz):
        ref = slot(item, zz, 1 - c)
        pltpu.make_async_remote_copy(
            ref, ref, ss.at[item, zz, 2], prs.at[item, zz], device_id=partner, device_id_type=MESH
        ).wait_recv()

    def own_moves(item, act):
        @pl.when(has_up)
        def _():
            act(chain(item, z, 0))

        if item not in (KEY, VAL):
            @pl.when(has_down)
            def _():
                act(chain(item, z, 1))

        if item in (KEY, VAL):
            @pl.when(c == 0)
            def _():
                act(chain(item, z, 2))
        elif item != WO:
            act(chain(item, z, 2))

    def passed_moves(item, k, below, act):
        zz = z - k if below else z + k
        if below:
            @pl.when(has_up)
            def _():
                act(chain(item, zz, 0))
        else:
            @pl.when(has_down)
            def _():
                act(chain(item, zz, 1))
        if item != WO:
            act(chain(item, zz, 2))

    def start(copy):
        copy.start()

    def wait_send(copy):
        copy.wait_send()

    def wo_block(g, cc):
        return wof.at[pl.ds(pl.multiple_of(cc * nout, 16), nout), pl.ds(pl.multiple_of(g * HD, HD), HD)]

    def in_plane(zz):
        return pltpu.make_async_remote_copy(
            woc.at[zz], wo_block(t, c), wi_ss.at[zz], wi_rs.at[t],
            device_id={"dp": dp, "tp": zz}, device_id_type=MESH,
        )

    def take_wo(zz):
        @pl.when(zz != t)
        def _():
            in_plane(zz).start()

        @pl.when(zz == t)
        def _():
            wo_block(t, c)[...] = woc[zz]
            own_wo(zz).start()

    def own_wo(zz):
        return pltpu.make_async_remote_copy(
            woc.at[zz], wo_block(t, c), wp_ss.at[t], wp_rs.at[t],
            device_id=partner, device_id_type=MESH,
        )

    def pass_on(item, k):
        @pl.when(z - k >= 0)
        def _():
            from_chain(item, z - k)
            passed_moves(item, k, True, start)
            if item == WO:
                take_wo(z - k)

        if item not in (KEY, VAL):
            @pl.when(z + k < nz)
            def _():
                from_chain(item, z + k)
                passed_moves(item, k, False, start)
                if item == WO:
                    take_wo(z + k)

    def each_side(k, fn):
        @pl.when(z - k >= 0)
        def _():
            fn(z - k)

        @pl.when(z + k < nz)
        def _():
            fn(z + k)

    def hidden_part(zz):
        return hid[:, pl.ds(pl.multiple_of(zz * 2 * shard, 128), 2 * shard)]

    def add_kv(zz):
        from_partner(KVA, zz)
        from_partner(KVB, zz)
        weights = wkv[pl.ds(pl.multiple_of(zz * 2 * shard, 16), 2 * shard), :]
        kvacc[...] += jnp.dot(hidden_part(zz), weights, preferred_element_type=jnp.float32)

    def add_q(zz):
        from_partner(WQ, zz)
        weights = wq[pl.ds(pl.multiple_of(zz * 2 * shard, 16), 2 * shard), :]
        qacc[...] += jnp.dot(hidden_part(zz), weights, preferred_element_type=jnp.float32)

    loads[0].wait()
    own_moves(KVA, start)
    own_moves(KVB, start)
    loads[2].wait()
    kvacc[...] = jnp.zeros_like(kvacc)
    qacc[...] = jnp.zeros_like(qacc)
    add_kv(z)
    for k in range(1, nz):
        pass_on(KVA, k)
        pass_on(KVB, k)
        if k == nz - 1:
            loads[1].wait()
            own_moves(WQ, start)
            loads[3].wait()
            own_moves(WO, start)
            take_wo(z)
        each_side(k, add_kv)

    role = t // (nt // 2)
    for h in range(2):
        kvloc[h] = kvacc[:, h * HD:(h + 1) * HD].astype(jnp.bfloat16)

    def kv_send(h):
        return pltpu.make_async_remote_copy(
            kvloc.at[h], kvb.at[dp, role], kv_ss.at[h], kv_rs.at[role],
            device_id={"dp": dp, "tp": 2 * (t % (nt // 2)) + h}, device_id_type=MESH,
        )

    for h in range(2):
        to = 2 * (t % (nt // 2)) + h

        @pl.when(to != t)
        def _():
            kv_send(h).start()

        @pl.when(to == t)
        def _():
            kvb[dp, role] = kvloc[h]

    add_q(z)
    for k in range(1, nz):
        pass_on(WQ, k)
        if k == 1:
            for r in range(2):
                @pl.when(t // 2 + r * (nt // 2) != t)
                def _():
                    pltpu.make_async_remote_copy(
                        kvloc.at[r], kvb.at[dp, r], kv_ss.at[r], kv_rs.at[r],
                        device_id=partner, device_id_type=MESH,
                    ).wait_recv()

            own_moves(KEY, start)
            own_moves(VAL, start)

            @pl.when(c == 0)
            def _():
                kvb[dp + 1] = jnp.zeros(kvb.shape[1:], kvb.dtype)

        pass_on(WO, k)
        each_side(k, add_q)
    qbuf[...] = (qacc[...] * (HD ** -0.5)).astype(jnp.bfloat16)

    qpos = dp * rows + lax.broadcasted_iota(jnp.int32, (rows, 1), 0)
    first = jnp.zeros((rows, 1), jnp.int32)
    end = jnp.int32(0)
    for r in range(lens_ref.shape[0]):
        end = end + lens_ref[r]
        first = jnp.where(qpos >= end, end, first)

    def pair(zz, which):
        return jnp.concatenate([kvb[2 * zz, which], kvb[2 * zz + 1, which]], axis=0)

    def score(zz):
        s = lax.dot_general(
            qbuf[...], pair(zz, 0), (((1,), (1,)), ((), ())), preferred_element_type=jnp.float32
        )
        kpos = zz * 2 * rows + lax.broadcasted_iota(jnp.int32, s.shape, 1)
        s = jnp.where((kpos >= first) & (kpos <= qpos), s, jnp.float32(-1e30))
        scores[zz] = s
        mref[...] = jnp.maximum(mref[...], jnp.max(s, axis=1, keepdims=True))

    mref[...] = jnp.full_like(mref, -1e30)
    for k in range(nz):
        if k == 0:
            @pl.when(c == 1)
            def _():
                from_partner(KEY, z)
            score(z)
        else:
            pass_on(KEY, k)
            pass_on(VAL, k)

            @pl.when(z - k >= 0)
            def _():
                from_partner(KEY, z - k)
                score(z - k)

    lref[...] = jnp.zeros_like(lref)
    oacc[...] = jnp.zeros_like(oacc)

    def weigh(zz, k):
        if k > 0:
            from_partner(VAL, zz)
        else:
            @pl.when(c == 1)
            def _():
                from_partner(VAL, zz)
        p = jnp.exp(scores[zz] - mref[...])
        lref[...] += jnp.sum(p, axis=1, keepdims=True)
        oacc[...] += jnp.dot(p.astype(jnp.bfloat16), pair(zz, 1), preferred_element_type=jnp.float32)

    for k in range(nz):
        @pl.when(z - k >= 0)
        def _():
            weigh(z - k, k)

    def head_cols(g):
        return hcat.at[:, pl.ds(pl.multiple_of(g * HD, HD), HD)]

    heads = (oacc[...] / lref[...]).astype(jnp.bfloat16)
    hloc[...] = heads
    head_cols(t)[...] = heads

    def head_copy(k):
        return pltpu.make_async_remote_copy(
            hloc, head_cols(t), h_ss.at[k], h_rs.at[t],
            device_id={"dp": dp, "tp": (t + k) % nt}, device_id_type=MESH,
        )

    for k in range(1, nt):
        head_copy(k).start()

    def wo_partner(g):
        return pltpu.make_async_remote_copy(
            wo_block(g, c), wo_block(g, c), wp_ss.at[g], wp_rs.at[g],
            device_id=partner, device_id_type=MESH,
        )

    for k in range(1, nt):
        g = (t + k) % nt
        pltpu.make_async_remote_copy(
            woc.at[0], wo_block(g, c), wi_ss.at[0], wi_rs.at[g],
            device_id=partner, device_id_type=MESH,
        ).wait_recv()
        wo_partner(g).start()
    for g in range(nt):
        pltpu.make_async_remote_copy(
            woc.at[0], wo_block(g, 1 - c), wp_ss.at[g], wp_rs.at[g],
            device_id=partner, device_id_type=MESH,
        ).wait_recv()
    for k in range(1, nt):
        g = (t + k) % nt
        pltpu.make_async_remote_copy(
            hloc, head_cols(g), h_ss.at[k], h_rs.at[g], device_id=partner, device_id_type=MESH
        ).wait_recv()
    out_ref[...] = lax.dot_general(
        hcat[...], wof[...], (((1,), (1,)), ((), ())), preferred_element_type=jnp.float32
    ).astype(out_ref.dtype)

    for item in (KVA, KVB, WQ, WO, KEY, VAL):
        own_moves(item, wait_send)
        for k in range(1, nz):
            @pl.when(z - k >= 0)
            def _():
                passed_moves(item, k, True, wait_send)

            if item not in (KEY, VAL):
                @pl.when(z + k < nz)
                def _():
                    passed_moves(item, k, False, wait_send)
    for h in range(2):
        @pl.when(2 * (t % (nt // 2)) + h != t)
        def _():
            kv_send(h).wait_send()
    for k in range(1, nt):
        head_copy(k).wait_send()
        wo_partner((t + k) % nt).wait_send()
        in_plane((t + k) % nt).wait_send()
    own_wo(t).wait_send()


def fused_body(nz, nt, hidden_states, resp_lengths, w_query, w_keyval, w_out):
    rows, depth = hidden_states.shape
    nout = w_out.shape[1]
    bf16, f32 = jnp.bfloat16, jnp.float32
    dma = pltpu.SemaphoreType.DMA
    hbm = pl.BlockSpec(memory_space=pltpu.HBM)
    return pl.pallas_call(
        functools.partial(fused_kernel, nz, nt),
        out_shape=jax.ShapeDtypeStruct((rows, 2 * nout), bf16),
        in_specs=[pl.BlockSpec(memory_space=pltpu.SMEM), hbm, hbm, hbm, hbm],
        out_specs=pl.BlockSpec(memory_space=pltpu.VMEM),
        scratch_shapes=[
            pltpu.VMEM((rows, depth), bf16),
            pltpu.VMEM((depth, w_query.shape[1]), bf16),
            pltpu.VMEM((depth, w_keyval.shape[1]), bf16),
            pltpu.VMEM((nz, nout, HD), bf16),
            pltpu.VMEM((2 * nout, nt * HD), bf16),
            pltpu.VMEM((2, rows, HD), bf16),
            pltpu.VMEM((2 * nz, 2, rows, HD), bf16),
            pltpu.VMEM((rows, 2 * HD), f32),
            pltpu.VMEM((rows, HD), f32),
            pltpu.VMEM((rows, HD), bf16),
            pltpu.VMEM((nz, rows, 2 * rows), f32),
            pltpu.VMEM((rows, 1), f32),
            pltpu.VMEM((rows, 1), f32),
            pltpu.VMEM((rows, HD), f32),
            pltpu.VMEM((rows, HD), bf16),
            pltpu.VMEM((rows, nt * HD), bf16),
            dma((4,)),
            dma((6, nz, 3)),
            dma((6, nz)),
            dma((6, nz)),
            dma((2,)),
            dma((2,)),
            dma((nz,)),
            dma((nt,)),
            dma((nt,)),
            dma((nt,)),
            dma((nt,)),
            dma((nt,)),
        ],
        compiler_params=pltpu.CompilerParams(
            collective_id=0, has_side_effects=True, vmem_limit_bytes=67_000_000
        ),
    )(resp_lengths, hidden_states, w_query, w_keyval, w_out.T)


def per_device(mesh, hidden_states, resp_lengths, w_query, w_keyval, w_out):
    nt = mesh.shape["tp"]
    nz = mesh.shape["dp"] // 2
    args = (hidden_states, resp_lengths, w_query, w_keyval, w_out)
    fits = (
        mesh.shape["dp"] == 2 * nz and nz == nt and nt % 2 == 0
        and w_query.shape[1] == HD and w_keyval.shape[1] == 2 * HD
        and w_out.shape[0] == HD and w_query.shape[0] % 64 == 0
    )
    return fused_body(nz, nt, *args) if fits else body(*args)


def solution(mesh):
    return jax.shard_map(
        functools.partial(per_device, mesh),
        mesh=mesh,
        in_specs=(P("dp", None), P(), P("dp", "tp"), P("dp", "tp"), P("tp", "dp")),
        out_specs=P("dp", "tp"),
        check_vma=False,
    )
```
